32 devices in a mesh: sub: 8 (over z, x), tile: 4 (over y, core).
Axes of the slice: x: 2, y: 2, z: 4, core: 2. Of those that a mesh axis runs over, the one named last changes fastest.
Arguments:
- coupling: bfloat16 [8, 28, 256, 256], P('sub'), may hold values from -0.125 to 0.125
- panel_inv: float32 [8, 8, 256, 256], P('sub')
- a_ib: bfloat16 [8, 2048, 3072], P('sub', None, 'tile'), may hold values from -0.5 to 0.5
- owner: int32 [8, 12, 12], P('sub', None, 'tile'), may hold values from 0 to 7, as said below
- slot: int32 [8, 12, 12], P('sub', None, 'tile'), may hold values from 0 to 15
- base: bfloat16 [8, 64, 256, 256], P('sub', 'tile'), may hold values from -2 to 2
Outputs:
- assembled: bfloat16 [8, 64, 256, 256], P('sub', 'tile')
The draws below stay inside these ranges and needn't reach their ends.
Inputs may be any that keep to these rules, and one draw needn't show every extreme that they name: `owner`: tiles of one device are those of one subdomain s and tile columns t*12/4 to (t+1)*12/4 - 1. At most 5 tiles of one device name one sub index; for each t one sub index, drawn from the seed, is named by exactly 5 tiles of every device of that t.
All inputs are finite; a program needn't handle non-finite values.
Results may differ from the reference program's by a relative error of at most 0.0051.
Values may be sent and summed in bfloat16 or wider, within the bound.
A program may use at most 128 MiB of HBM per device.

```python
import math
import jax
import jax.numpy as jnp
from jax import lax

NI = 2048
NB = 3072
PANEL = 256
SLOTS = 16
LOWER = 28
NBT = 12
SUBS = 8
OWNED = 64
N_SUB = 8
N_TILE = 4


def draw_panel_inv(key, part):
    random_key = jax.random.fold_in(key, 1)
    shape = (SUBS, NI // PANEL, PANEL, PANEL)
    random_part = jax.random.normal(random_key, shape, jnp.float32)
    identity = jnp.eye(PANEL, dtype=jnp.float32)
    return 0.6 * identity + 0.3 * random_part / math.sqrt(PANEL)


def draw_owner(key, part):
    tile_side = NB // PANEL
    tile_count = tile_side * tile_side // N_TILE
    capacity = (tile_count + N_SUB - 1) // N_SUB
    others = (N_SUB - 1) * capacity
    hot_key, seat_key = jax.random.split(key)
    hottest = jax.random.randint(hot_key, (N_TILE,), 0, N_SUB).astype(jnp.int32)

    def one_device(device_key, hot_owner):
        first_key, second_key = jax.random.split(device_key)
        seat_order = jax.random.permutation(first_key, others)[:tile_count - capacity].astype(jnp.int32)
        chosen = (hot_owner + 1 + seat_order // capacity) % N_SUB
        listed = jnp.concatenate([jnp.full((capacity,), hot_owner, jnp.int32), chosen.astype(jnp.int32)])
        return listed[jax.random.permutation(second_key, tile_count)]
    device_keys = jax.random.split(seat_key, SUBS * N_TILE)
    hot_all = jnp.tile(hottest, SUBS)
    drawn = jax.vmap(one_device)(device_keys, hot_all)
    drawn = drawn.reshape(SUBS, N_TILE, tile_side, tile_count // tile_side)
    return drawn.transpose(0, 2, 1, 3).reshape(SUBS, tile_side, tile_side)


def set_ends(array, rng, least, high):
    extent = array.shape
    index_at = [jax.random.randint(jax.random.fold_in(rng, axis), (), 0, extent[axis]) for axis in range(len(extent))]
    array = array.at[tuple(index_at)].set(least)
    longest = extent.index(max(extent))
    index_at[longest] = (index_at[longest] + 1) % extent[longest]
    return array.at[tuple(index_at)].set(high)


def level_of(stream_key, dims, cuts, low, top_value):
    loudness, own = 1.0, jax.random.fold_in(stream_key, 6)
    for axis_at, parts in cuts:
        steps = jnp.exp(jax.random.uniform(jax.random.fold_in(own, axis_at), (parts,), jnp.float32, low / len(cuts), top_value / len(cuts)))
        loudness = loudness * jnp.repeat(steps, dims[axis_at] // parts).reshape([-1 if axis == axis_at else 1 for axis in range(len(dims))])
    return loudness


def scatter_about(key, shape, scale, most, pieces=(), kind=jnp.bfloat16):
    values = scale * jax.random.normal(key, shape, jnp.float32)
    if pieces:
        values = values * level_of(key, shape, pieces, -0.22, 0.18)
    return jnp.clip(values, -most, most).astype(kind)


def setup_inputs(seed: int = 0) -> dict:
    key_of = jax.random.split(jax.random.key(seed), 7)
    coupling = scatter_about(key_of[0], (SUBS, LOWER, PANEL, PANEL), NI ** -0.5, 0.125, ((0, 8),))
    panel_inv = draw_panel_inv(jax.random.fold_in(key_of[6], 71), 0)
    a_ib = scatter_about(key_of[2], (SUBS, NI, NB), 0.0625, 0.5, ((0, 8), (2, 4)))
    owner = draw_owner(jax.random.fold_in(key_of[6], 71), 0)
    slot = set_ends(jax.random.randint(key_of[4], (SUBS, NBT, NBT), 0, SLOTS), jax.random.fold_in(key_of[4], 1), 0, SLOTS - 1).astype(jnp.int32)
    base = scatter_about(key_of[5], (SUBS, OWNED, PANEL, PANEL), 0.3, 2.0, ((0, 8), (1, 4)))
    return dict(coupling=coupling, panel_inv=panel_inv, a_ib=a_ib, owner=owner, slot=slot, base=base)


def solve(lower_blocks, inverse, right_cols):
    panel_width = inverse.shape[1]
    panels = []
    for row_panel in range(inverse.shape[0]):
        target = right_cols[row_panel * panel_width:(row_panel + 1) * panel_width].astype(jnp.float32)
        if row_panel > 0:
            block_start = row_panel * (row_panel - 1) // 2
            blocks = lower_blocks[block_start:block_start + row_panel]
            joined = jnp.transpose(blocks, (1, 0, 2)).reshape(panel_width, row_panel * panel_width)
            target = target - jnp.dot(joined, jnp.concatenate(panels, axis=0), preferred_element_type=jnp.float32)
        solved_panel = jnp.dot(inverse[row_panel], target, precision=lax.Precision.HIGHEST, preferred_element_type=jnp.float32)
        panels.append(solved_panel.astype(jnp.bfloat16))
    return jnp.concatenate(panels, axis=0)


def reference(coupling, panel_inv, a_ib, owner, slot, base):
    tile_side = NB // PANEL
    col_tiles = tile_side // N_TILE
    column_group = jnp.arange(tile_side, dtype=jnp.int32) // col_tiles

    def assemble_one(accumulated, operands):
        lower_blocks, inverse, right_cols, owner_ids, slot_ids = operands
        solved = solve(lower_blocks, inverse, right_cols)
        gram_matrix = lax.dot_general(solved, solved, (((0,), (0,)), ((), ())), preferred_element_type=jnp.float32)
        contrib = (-gram_matrix).astype(jnp.bfloat16)
        contrib = lax.optimization_barrier(contrib).astype(jnp.float32)
        tiled = contrib.reshape(tile_side, PANEL, tile_side, PANEL).transpose(0, 2, 1, 3)
        places = column_group[None, :] * SLOTS + slot_ids
        accumulated = accumulated.at[owner_ids, places].add(tiled)
        return accumulated, None

    start_total = jnp.zeros((SUBS, OWNED, PANEL, PANEL), jnp.float32)
    accumulated, _ = lax.scan(assemble_one, start_total, (coupling, panel_inv, a_ib, owner, slot))
    return (base.astype(jnp.float32) + accumulated).astype(jnp.bfloat16)
```

```python
import functools

import jax
import jax.numpy as jnp
from jax import lax
from jax.experimental import pallas as pl
from jax.experimental.pallas import tpu as pltpu
from jax.sharding import PartitionSpec as P

MESH = pl.DeviceIdType.MESH
F32 = jnp.float32
BF16 = jnp.bfloat16
GROUP = 8


def flip(value, bit, on):
    return value + on * (bit - 2 * bit * ((value // bit) % 2))


def flip_mask(value, mask):
    for bit in (1, 2, 4):
        value = flip(value, bit, (mask // bit) % 2)
    return value


def inner_order(i):
    high = i // 4
    first = 5 - 2 * (i % 2) - i // 2
    last = 7 - (i - 4) - 4 * ((i - 4) // 2)
    return (1 - high) * first + high * last


def kernel(
    dims,
    meta_sm,
    meta_any,
    coupling_hbm,
    inverse_hbm,
    cols_hbm,
    base_hbm,
    result,
    metas,
    coupling,
    inverse,
    cols,
    base,
    held,
    detour,
    packed,
    incoming,
    total,
    table,
    labels,
    meta_all,
    load_sem,
    own_send,
    own_recv,
    relay_send,
    relay_recv,
    detour_send,
    detour_recv,
    forward_send,
    forward_recv,
    out_send,
    out_recv,
    meta_send,
    meta_recv,
    local_sem,
):
    n_sub, n_tile, panels, width, col_tiles, tile_count, capacity, slots = dims
    me = lax.axis_index("sub")
    col = lax.axis_index("tile")
    rows = tile_count // col_tiles
    half_tile = n_tile // 2
    partner = col + 1 - 2 * (col % 2)
    across = (col + half_tile) % n_tile
    groups = n_sub // GROUP
    group = me // GROUP
    within = me % GROUP
    inner = ((within // 2 + 1) % 4) // 2
    mate = flip(me, 2, 1)
    detoured = [k for k in range(panels) if k % 2 == 1][: panels * 3 // 8]
    direct = [k for k in range(panels) if k not in detoured]

    def send_mask(step):
        place = step % GROUP
        return inner * inner_order(place) + (1 - inner) * (GROUP - 1 - place)

    def send_peer(step):
        mask = send_mask(step)
        return ((group + 1 + step // GROUP) % groups) * GROUP + flip_mask(within, mask)

    def slot_at(step, peer, mask):
        role = ((peer % GROUP // 2 + 1) % 4) // 2
        some = (mask + GROUP - 1) // GROUP
        at = (8 + 4 * role - mask) % (GROUP - 1)
        return step // GROUP * GROUP + some * at + (1 - some) * (GROUP - 1)

    def source_peer(step):
        place = step % GROUP
        some = 1 - place // (GROUP - 1)
        mask = some * ((7 + 4 * inner - place) % (GROUP - 1) + 1)
        return ((group + 2 * groups - 1 - step // GROUP) % groups) * GROUP + flip_mask(within, mask)

    loads = [
        pltpu.make_async_copy(cols_hbm.at[0], cols.at[0], load_sem.at[0]),
        pltpu.make_async_copy(inverse_hbm.at[0], inverse.at[0], load_sem.at[1]),
        pltpu.make_async_copy(coupling_hbm, coupling, load_sem.at[2]),
        pltpu.make_async_copy(
            inverse_hbm.at[pl.ds(1, panels - 1)], inverse.at[pl.ds(1, panels - 1)], load_sem.at[3]
        ),
        pltpu.make_async_copy(
            cols_hbm.at[pl.ds(1, panels - 1)], cols.at[pl.ds(1, panels - 1)], load_sem.at[4]
        ),
    ]
    for load in loads:
        load.start()
    base_load = pltpu.make_async_copy(base_hbm, base, load_sem.at[5])
    base_load.start()

    barrier = pltpu.get_barrier_semaphore()
    for place in (partner, across):
        pl.semaphore_signal(barrier, inc=1, device_id={"tile": place}, device_id_type=MESH)
    pl.semaphore_signal(
        barrier, inc=1, device_id={"sub": mate, "tile": across}, device_id_type=MESH
    )

    @pl.loop(1, n_sub)
    def _(j):
        pl.semaphore_signal(
            barrier, inc=1, device_id={"sub": (me + j) % n_sub}, device_id_type=MESH
        )

    def block(where, k):
        return held.at[where * panels + k]

    def solve_panel(k):
        start = k * (k - 1) // 2
        inv = inverse[k]
        inv_high = inv.astype(BF16)
        inv_low = (inv - inv_high.astype(F32)).astype(BF16)
        for i in range(col_tiles):
            value = cols[k, :, i * width : (i + 1) * width].astype(F32)
            if k:
                value -= sum(
                    jnp.dot(
                        coupling[start + m],
                        held[col * panels + m, i],
                        preferred_element_type=F32,
                    )
                    for m in range(k)
                )
            high = value.astype(BF16)
            low = (value - high.astype(F32)).astype(BF16)
            answer = jnp.dot(inv_high, low, preferred_element_type=F32)
            answer += jnp.dot(inv_low, high, preferred_element_type=F32)
            answer += jnp.dot(inv_high, high, preferred_element_type=F32)
            held[col * panels + k, i] = answer.astype(BF16)

    def own_copy(k, way):
        return pltpu.make_async_remote_copy(
            src_ref=block(col, k),
            dst_ref=block(col, k),
            send_sem=own_send.at[way, k],
            recv_sem=own_recv.at[way, k],
            device_id={"tile": (partner, across)[way]},
            device_id_type=MESH,
        )

    def relay_copy(k):
        return pltpu.make_async_remote_copy(
            src_ref=block(across, k),
            dst_ref=block(across, k),
            send_sem=relay_send.at[k],
            recv_sem=relay_recv.at[k],
            device_id={"tile": partner},
            device_id_type=MESH,
        )

    def detour_copy(j):
        return pltpu.make_async_remote_copy(
            src_ref=block(col, detoured[j]),
            dst_ref=detour.at[j],
            send_sem=detour_send.at[j],
            recv_sem=detour_recv.at[j],
            device_id={"sub": mate, "tile": across},
            device_id_type=MESH,
        )

    def forward_copy(j):
        return pltpu.make_async_remote_copy(
            src_ref=detour.at[j],
            dst_ref=block(across, detoured[j]),
            send_sem=forward_send.at[j],
            recv_sem=forward_recv.at[j],
            device_id={"sub": mate},
            device_id_type=MESH,
        )

    def out_copy(step, r, peer, at):
        return pltpu.make_async_remote_copy(
            src_ref=packed.at[step, r],
            dst_ref=incoming.at[at, r],
            send_sem=out_send.at[step, r],
            recv_sem=out_recv.at[at, r],
            device_id={"sub": peer},
            device_id_type=MESH,
        )

    def meta_copy(peer, source):
        return pltpu.make_async_remote_copy(
            src_ref=meta_any,
            dst_ref=metas.at[source],
            send_sem=meta_send.at[peer],
            recv_sem=meta_recv.at[source],
            device_id={"sub": peer},
            device_id_type=MESH,
        )

    def start_panel(k):
        own_copy(k, 0).start()

        @pl.when(inner == 0)
        def _():
            if k in detoured:
                detour_copy(detoured.index(k)).start()
            else:
                own_copy(k, 1).start()

    loads[0].wait()
    loads[1].wait()
    solve_panel(0)
    pl.semaphore_wait(barrier, n_sub + 2)
    start_panel(0)
    for load in loads[2:]:
        load.wait()
    for k in range(1, panels):
        solve_panel(k)
        start_panel(k)

    @pl.loop(1, n_sub)
    def _(j):
        meta_copy((me + j) % n_sub, me).start()

    own_meta = pltpu.make_async_copy(meta_any, meta_all.at[me], local_sem.at[1])
    own_meta.start()

    def pick(read, low, default, value_of, store):
        def body(i, carry):
            count, chosen = carry
            value = read(i)
            hit = (value >= low) & (value < low + slots)
            new = value_of(i, value)
            chosen = tuple(
                jnp.where(hit & (count == r), new, c) for r, c in enumerate(chosen)
            )
            return count + jnp.where(hit, 1, 0), chosen

        start = (jnp.int32(0), tuple(jnp.int32(default) for _ in range(capacity)))
        _, chosen = lax.fori_loop(0, tile_count, body, start)
        for r, c in enumerate(chosen):
            store(r, c)

    @pl.loop(0, n_sub)
    def _(d):
        def store(r, c):
            table[d * capacity + r] = c

        pick(lambda i: meta_sm[0, i], d * slots, 0, lambda i, v: i, store)

    @pl.when(inner == 1)
    def _():
        for j in range(len(detoured)):
            detour_copy(j).wait_recv()
            forward_copy(j).start()
        for k in range(panels):
            own_copy(k, 1).start()

    @pl.loop(1, n_sub)
    def _(j):
        source = (me + j) % n_sub
        meta_copy(source, source).wait_recv()
        fetch = pltpu.make_async_copy(metas.at[source], meta_all.at[source], local_sem.at[2])
        fetch.start()
        fetch.wait()

    own_meta.wait()

    @pl.loop(0, n_sub)
    def _(s):
        def store(r, c):
            labels[s * capacity + r] = c

        pick(
            lambda i: meta_all[s, 0, i], me * slots, slots, lambda i, v: v - me * slots, store
        )

    base_load.wait()

    @pl.loop(0, slots)
    def _(q):
        total[q] = base[q].astype(F32)

    @pl.when(inner == 0)
    def _():
        for k in sorted(range(panels), key=lambda k: k + (1.5 if k in detoured else 0)):
            if k in detoured:
                forward_copy(detoured.index(k)).wait_recv()
            else:
                own_copy(k, 1).wait_recv()
            relay_copy(k).start()

    @pl.when(inner == 1)
    def _():
        for k in range(panels):
            own_copy(k, 1).wait_recv()
            relay_copy(k).start()

    for k in range(panels):
        own_copy(k, 0).wait_recv()
        relay_copy(k).wait_recv()

    def tile_of(entry):
        right = entry // rows
        left = entry % rows
        place = left // col_tiles
        product = sum(
            lax.dot_general(
                held[place * panels + k, left % col_tiles],
                held[col * panels + k, right],
                (((0,), (0,)), ((), ())),
                preferred_element_type=F32,
            )
            for k in range(panels)
        )
        return (-product).astype(BF16)

    @pl.loop(0, n_sub - 1)
    def _(step):
        peer = send_peer(step)
        for r in range(capacity):
            packed[step, r] = tile_of(table[peer * capacity + r])
            out_copy(step, r, peer, slot_at(step, peer, send_mask(step))).start()

    for r in range(capacity):
        packed[n_sub - 1, r] = tile_of(table[me * capacity + r])

    strip = 32

    def gather(tiles, source):
        wanted = [labels[source * capacity + r] for r in range(capacity)]
        for c in range(width // strip):
            at = slice(c * strip, (c + 1) * strip)
            parts = [tiles(r, at).astype(F32) for r in range(capacity)]

            @pl.loop(0, slots)
            def _(q):
                value = total[q, at]
                for r in range(capacity):
                    value += jnp.where(wanted[r] == q, parts[r], 0.0)
                total[q, at] = value

    gather(lambda r, at: packed[n_sub - 1, r, at], me)

    @pl.loop(0, n_sub - 1)
    def _(step):
        source = source_peer(step)
        for r in range(capacity):
            out_copy(step, r, source, step).wait_recv()
        gather(lambda r, at: incoming[step, r, at], source)

    @pl.loop(0, slots)
    def _(q):
        result[q] = total[q].astype(BF16)

    for k in range(panels):
        own_copy(k, 0).wait_send()
        relay_copy(k).wait_send()

    @pl.when(inner == 0)
    def _():
        for k in direct:
            own_copy(k, 1).wait_send()
        for j in range(len(detoured)):
            detour_copy(j).wait_send()

    @pl.when(inner == 1)
    def _():
        for k in range(panels):
            own_copy(k, 1).wait_send()
        for j in range(len(detoured)):
            forward_copy(j).wait_send()

    @pl.loop(1, n_sub)
    def _(j):
        source = (me + j) % n_sub
        meta_copy(source, source).wait_send()

    @pl.loop(0, n_sub - 1)
    def _(step):
        for r in range(capacity):
            out_copy(step, r, me, step).wait_send()


def shards(coupling, panel_inv, a_ib, owner, slot, base):
    lower_blocks = coupling[0]
    inverse = panel_inv[0]
    panels, width = inverse.shape[:2]
    col_count = a_ib.shape[2]
    right_cols = a_ib[0].reshape(panels, width, col_count)
    n_sub = lax.axis_size("sub")
    n_tile = lax.axis_size("tile")
    assert n_tile == 4 and n_sub % GROUP == 0
    col_tiles = col_count // width
    tile_count = owner.shape[1] * owner.shape[2]
    assert owner.shape[1] == n_tile * col_tiles
    capacity = (tile_count + n_sub - 1) // n_sub
    slots = base.shape[1]
    room = (tile_count + 127) // 128 * 128
    meta = (owner[0] * slots + slot[0]).T.reshape(1, tile_count)
    meta = jnp.pad(meta, ((0, 0), (0, room - tile_count)))
    dims = (n_sub, n_tile, panels, width, col_tiles, tile_count, capacity, slots)
    relayed = panels * 3 // 8
    any_spec = pl.BlockSpec(memory_space=pl.ANY)
    smem_spec = pl.BlockSpec(memory_space=pltpu.SMEM)
    dma = pltpu.SemaphoreType.DMA
    result, _ = pl.pallas_call(
        functools.partial(kernel, dims),
        out_shape=(
            jax.ShapeDtypeStruct((slots, width, width), BF16),
            jax.ShapeDtypeStruct((n_sub, 1, room), jnp.int32),
        ),
        in_specs=[smem_spec, any_spec, any_spec, any_spec, any_spec, any_spec],
        out_specs=(pl.BlockSpec(memory_space=pltpu.VMEM), any_spec),
        scratch_shapes=[
            pltpu.VMEM(lower_blocks.shape, BF16),
            pltpu.VMEM(inverse.shape, F32),
            pltpu.VMEM(right_cols.shape, BF16),
            pltpu.VMEM((slots, width, width), BF16),
            pltpu.VMEM((n_tile * panels, col_tiles, width, width), BF16),
            pltpu.VMEM((relayed, col_tiles, width, width), BF16),
            pltpu.VMEM((n_sub, capacity, width, width), BF16),
            pltpu.VMEM((n_sub - 1, capacity, width, width), BF16),
            pltpu.VMEM((slots, width, width), F32),
            pltpu.SMEM((n_sub * capacity,), jnp.int32),
            pltpu.SMEM((n_sub * capacity,), jnp.int32),
            pltpu.SMEM((n_sub, 1, room), jnp.int32),
            dma((6,)),
            dma((2, panels)),
            dma((2, panels)),
            dma((panels,)),
            dma((panels,)),
            dma((relayed,)),
            dma((relayed,)),
            dma((relayed,)),
            dma((relayed,)),
            dma((n_sub, capacity)),
            dma((n_sub, capacity)),
            dma((n_sub,)),
            dma((n_sub,)),
            dma((3,)),
        ],
        compiler_params=pltpu.CompilerParams(
            collective_id=0, has_side_effects=True, vmem_limit_bytes=62 * 1024 * 1024
        ),
    )(meta, meta, lower_blocks, inverse, right_cols, base[0])
    return result[None]


def solution(mesh):
    placed = (
        P("sub", None, None, None),
        P("sub", None, None, None),
        P("sub", None, "tile"),
        P("sub", None, "tile"),
        P("sub", None, "tile"),
        P("sub", "tile", None, None),
    )
    return jax.shard_map(
        shards, mesh=mesh, in_specs=placed, out_specs=P("sub", "tile", None, None), check_vma=False
    )
```

```python
import functools

import jax
import jax.numpy as jnp
from jax import lax
from jax.experimental import pallas as pl
from jax.experimental.pallas import tpu as pltpu
from jax.sharding import PartitionSpec as P

MESH = pl.DeviceIdType.MESH
F32 = jnp.float32
BF16 = jnp.bfloat16
GROUP = 8


def flip(value, bit, on):
    return value + on * (bit - 2 * bit * ((value // bit) % 2))


def flip_mask(value, mask):
    for bit in (1, 2, 4):
        value = flip(value, bit, (mask // bit) % 2)
    return value


def inner_order(i):
    high = i // 4
    first = 5 - 2 * (i % 2) - i // 2
    last = 7 - (i - 4) - 4 * ((i - 4) // 2)
    return (1 - high) * first + high * last


def detour_chunks(chunks):
    return list(range(1, chunks, 2))[: chunks * 10 // 24]


def kernel(
    dims,
    meta_sm,
    meta_any,
    coupling_hbm,
    inverse_hbm,
    cols_hbm,
    base_hbm,
    result,
    metas,
    coupling,
    inverse,
    cols,
    base,
    ahead,
    held,
    detour,
    packed,
    incoming,
    total,
    table,
    labels,
    meta_all,
    load_sem,
    near_send,
    near_recv,
    own_send,
    own_recv,
    relay_send,
    relay_recv,
    detour_send,
    detour_recv,
    forward_send,
    forward_recv,
    out_send,
    out_recv,
    meta_send,
    meta_recv,
    local_sem,
):
    n_sub, n_tile, panels, width, col_tiles, tile_count, capacity, slots = dims
    me = lax.axis_index("sub")
    col = lax.axis_index("tile")
    rows = tile_count // col_tiles
    half_tile = n_tile // 2
    partner = col + 1 - 2 * (col % 2)
    across = (col + half_tile) % n_tile
    groups = n_sub // GROUP
    group = me // GROUP
    within = me % GROUP
    inner = ((within // 2 + 1) % 4) // 2
    mate = flip(me, 2, 1)
    chunks = panels * col_tiles
    detoured = detour_chunks(chunks)
    direct = [c for c in range(chunks) if c not in detoured]

    def send_mask(step):
        place = step % GROUP
        return inner * inner_order(place) + (1 - inner) * (GROUP - 1 - place)

    def send_peer(step):
        mask = send_mask(step)
        return ((group + 1 + step // GROUP) % groups) * GROUP + flip_mask(within, mask)

    def slot_at(step, peer, mask):
        role = ((peer % GROUP // 2 + 1) % 4) // 2
        some = (mask + GROUP - 1) // GROUP
        at = (8 + 4 * role - mask) % (GROUP - 1)
        return step // GROUP * GROUP + some * at + (1 - some) * (GROUP - 1)

    def source_peer(step):
        place = step % GROUP
        some = 1 - place // (GROUP - 1)
        mask = some * ((7 + 4 * inner - place) % (GROUP - 1) + 1)
        return ((group + 2 * groups - 1 - step // GROUP) % groups) * GROUP + flip_mask(within, mask)

    loads = [
        pltpu.make_async_copy(cols_hbm.at[0], cols.at[0], load_sem.at[0]),
        pltpu.make_async_copy(inverse_hbm.at[0], inverse.at[0], load_sem.at[1]),
        pltpu.make_async_copy(coupling_hbm, coupling, load_sem.at[2]),
        pltpu.make_async_copy(
            inverse_hbm.at[pl.ds(1, panels - 1)], inverse.at[pl.ds(1, panels - 1)], load_sem.at[3]
        ),
        pltpu.make_async_copy(
            cols_hbm.at[pl.ds(1, panels - 1)], cols.at[pl.ds(1, panels - 1)], load_sem.at[4]
        ),
    ]
    for load in loads:
        load.start()
    base_load = pltpu.make_async_copy(base_hbm, base, load_sem.at[5])
    base_load.start()

    barrier = pltpu.get_barrier_semaphore()
    for place in (partner, across):
        pl.semaphore_signal(barrier, inc=1, device_id={"tile": place}, device_id_type=MESH)
    pl.semaphore_signal(
        barrier, inc=1, device_id={"sub": mate, "tile": across}, device_id_type=MESH
    )

    @pl.loop(1, n_sub)
    def _(j):
        pl.semaphore_signal(
            barrier, inc=1, device_id={"sub": (me + j) % n_sub}, device_id_type=MESH
        )

    def block(where, k):
        return held.at[where * panels + k]

    def chunk(where, c):
        return held.at[where * panels + c // col_tiles, c % col_tiles]

    def update(k, i, value, sources):
        for m in sources:
            value -= jnp.dot(
                coupling[k * (k - 1) // 2 + m], held[col * panels + m, i], preferred_element_type=F32
            )
        return value

    def solve_panel(k):
        inv = inverse[k]
        inv_high = inv.astype(BF16)
        inv_low = (inv - inv_high.astype(F32)).astype(BF16)
        for i in range(col_tiles):
            if k > 1:
                value = ahead[k % 2, i]
            else:
                value = cols[k, :, i * width : (i + 1) * width].astype(F32)
            value = update(k, i, value, range(max(k - 1, 0), k))
            high = value.astype(BF16)
            low = (value - high.astype(F32)).astype(BF16)
            answer = jnp.dot(inv_high, low, preferred_element_type=F32)
            answer += jnp.dot(inv_low, high, preferred_element_type=F32)
            answer += jnp.dot(inv_high, high, preferred_element_type=F32)
            held[col * panels + k, i] = answer.astype(BF16)
        if 0 < k < panels - 1:
            for i in range(col_tiles):
                value = cols[k + 1, :, i * width : (i + 1) * width].astype(F32)
                ahead[(k + 1) % 2, i] = update(k + 1, i, value, range(k))

    def near_copy(k):
        return pltpu.make_async_remote_copy(
            src_ref=block(col, k),
            dst_ref=block(col, k),
            send_sem=near_send.at[k],
            recv_sem=near_recv.at[k],
            device_id={"tile": partner},
            device_id_type=MESH,
        )

    def own_copy(c):
        return pltpu.make_async_remote_copy(
            src_ref=chunk(col, c),
            dst_ref=chunk(col, c),
            send_sem=own_send.at[c],
            recv_sem=own_recv.at[c],
            device_id={"tile": across},
            device_id_type=MESH,
        )

    def relay_copy(c):
        return pltpu.make_async_remote_copy(
            src_ref=chunk(across, c),
            dst_ref=chunk(across, c),
            send_sem=relay_send.at[c],
            recv_sem=relay_recv.at[c],
            device_id={"tile": partner},
            device_id_type=MESH,
        )

    def detour_copy(j):
        return pltpu.make_async_remote_copy(
            src_ref=chunk(col, detoured[j]),
            dst_ref=detour.at[j],
            send_sem=detour_send.at[j],
            recv_sem=detour_recv.at[j],
            device_id={"sub": mate, "tile": across},
            device_id_type=MESH,
        )

    def forward_copy(j):
        return pltpu.make_async_remote_copy(
            src_ref=detour.at[j],
            dst_ref=chunk(across, detoured[j]),
            send_sem=forward_send.at[j],
            recv_sem=forward_recv.at[j],
            device_id={"sub": mate},
            device_id_type=MESH,
        )

    def out_copy(step, r, peer, at):
        return pltpu.make_async_remote_copy(
            src_ref=packed.at[step, r],
            dst_ref=incoming.at[at, r],
            send_sem=out_send.at[step, r],
            recv_sem=out_recv.at[at, r],
            device_id={"sub": peer},
            device_id_type=MESH,
        )

    def meta_copy(peer, source):
        return pltpu.make_async_remote_copy(
            src_ref=meta_any,
            dst_ref=metas.at[source],
            send_sem=meta_send.at[peer],
            recv_sem=meta_recv.at[source],
            device_id={"sub": peer},
            device_id_type=MESH,
        )

    def start_panel(k):
        @pl.when(inner == 0)
        def _():
            for c in range(k * col_tiles, (k + 1) * col_tiles):
                if c in detoured:
                    detour_copy(detoured.index(c)).start()
                else:
                    own_copy(c).start()

    loads[0].wait()
    loads[1].wait()
    for k in range(panels):
        if k == 1:
            for load in loads[2:]:
                load.wait()
        solve_panel(k)
        if k == 0:
            pl.semaphore_wait(barrier, n_sub + 2)
        start_panel(k)
        near_copy(k).start()

    @pl.loop(1, n_sub)
    def _(j):
        meta_copy((me + j) % n_sub, me).start()

    own_meta = pltpu.make_async_copy(meta_any, meta_all.at[me], local_sem.at[1])
    own_meta.start()

    def pick(read, low, default, value_of, store):
        def body(i, carry):
            count, chosen = carry
            for j in range(col_tiles):
                value = read(j, i)
                hit = (value >= low) & (value < low + slots)
                new = value_of(j * rows + i, value)
                chosen = tuple(
                    jnp.where(hit & (count == r), new, c) for r, c in enumerate(chosen)
                )
                count += jnp.where(hit, 1, 0)
            return count, chosen

        start = (jnp.int32(0), tuple(jnp.int32(default) for _ in range(capacity)))
        _, chosen = lax.fori_loop(0, rows, body, start)
        for r, c in enumerate(chosen):
            store(r, c)

    @pl.when(inner == 1)
    def _():
        for j in range(len(detoured)):
            detour_copy(j).wait_recv()
            forward_copy(j).start()
            if j == len(detoured) - 2:
                for c in range(chunks):
                    own_copy(c).start()

    @pl.loop(0, n_sub)
    def _(d):
        def store(r, c):
            table[d * capacity + r] = c

        pick(lambda j, i: meta_sm[j, i], d * slots, 0, lambda i, v: i, store)

    @pl.loop(1, n_sub)
    def _(j):
        source = (me + j) % n_sub
        meta_copy(source, source).wait_recv()
        fetch = pltpu.make_async_copy(metas.at[source], meta_all.at[source], local_sem.at[2])
        fetch.start()
        fetch.wait()

    own_meta.wait()

    @pl.loop(0, n_sub)
    def _(s):
        def store(r, c):
            labels[s * capacity + r] = c

        pick(
            lambda j, i: meta_all[s, j, i], me * slots, slots, lambda i, v: v - me * slots, store
        )

    base_load.wait()

    @pl.loop(0, slots)
    def _(q):
        total[q] = base[q].astype(F32)

    @pl.when(inner == 0)
    def _():
        arrivals = [(n, c) for n, c in enumerate(direct)]
        arrivals += [(n + 2.5, c) for n, c in enumerate(detoured)]
        for _, c in sorted(arrivals):
            if c in detoured:
                forward_copy(detoured.index(c)).wait_recv()
            else:
                own_copy(c).wait_recv()
            relay_copy(c).start()

    @pl.when(inner == 1)
    def _():
        for c in range(chunks):
            own_copy(c).wait_recv()
            relay_copy(c).start()

    for k in range(panels):
        near_copy(k).wait_recv()
    for c in range(chunks):
        relay_copy(c).wait_recv()

    def tile_of(entry):
        right = entry // rows
        left = entry % rows
        place = left // col_tiles
        product = sum(
            lax.dot_general(
                held[place * panels + k, left % col_tiles],
                held[col * panels + k, right],
                (((0,), (0,)), ((), ())),
                preferred_element_type=F32,
            )
            for k in range(panels)
        )
        return (-product).astype(BF16)

    @pl.loop(0, n_sub - 1)
    def _(step):
        peer = send_peer(step)
        for r in range(capacity):
            packed[step, r] = tile_of(table[peer * capacity + r])
            out_copy(step, r, peer, slot_at(step, peer, send_mask(step))).start()

    for r in range(capacity):
        packed[n_sub - 1, r] = tile_of(table[me * capacity + r])

    strip = 32

    def gather(tiles, source, picks, target):
        wanted = [labels[source * capacity + r] for r in picks]
        for c in range(width // strip):
            at = slice(c * strip, (c + 1) * strip)
            parts = [tiles(r, at).astype(F32) for r in picks]

            @pl.loop(0, slots)
            def _(q):
                value = total[q, at]
                for want, part in zip(wanted, parts):
                    value += jnp.where(want == q, part, 0.0)
                target[q, at] = value.astype(target.dtype)

    every = range(capacity)
    gather(lambda r, at: packed[n_sub - 1, r, at], me, every, total)

    @pl.loop(0, n_sub - 2)
    def _(step):
        source = source_peer(step)
        for r in every:
            out_copy(step, r, source, step).wait_recv()
        gather(lambda r, at: incoming[step, r, at], source, every, total)

    final = n_sub - 2
    source = source_peer(final)
    for r in every:
        out_copy(final, r, source, final).wait_recv()
        target = result if r == capacity - 1 else total
        gather(lambda r, at: incoming[final, r, at], source, [r], target)

    for k in range(panels):
        near_copy(k).wait_send()
    for c in range(chunks):
        relay_copy(c).wait_send()

    @pl.when(inner == 0)
    def _():
        for c in direct:
            own_copy(c).wait_send()
        for j in range(len(detoured)):
            detour_copy(j).wait_send()

    @pl.when(inner == 1)
    def _():
        for c in range(chunks):
            own_copy(c).wait_send()
        for j in range(len(detoured)):
            forward_copy(j).wait_send()

    @pl.loop(1, n_sub)
    def _(j):
        source = (me + j) % n_sub
        meta_copy(source, source).wait_send()

    @pl.loop(0, n_sub - 1)
    def _(step):
        for r in range(capacity):
            out_copy(step, r, me, step).wait_send()


def shards(coupling, panel_inv, a_ib, owner, slot, base):
    lower_blocks = coupling[0]
    inverse = panel_inv[0]
    panels, width = inverse.shape[:2]
    col_count = a_ib.shape[2]
    right_cols = a_ib[0].reshape(panels, width, col_count)
    n_sub = lax.axis_size("sub")
    n_tile = lax.axis_size("tile")
    assert n_tile == 4 and n_sub % GROUP == 0
    col_tiles = col_count // width
    tile_count = owner.shape[1] * owner.shape[2]
    assert owner.shape[1] == n_tile * col_tiles
    capacity = (tile_count + n_sub - 1) // n_sub
    slots = base.shape[1]
    meta = (owner[0] * slots + slot[0]).T
    dims = (n_sub, n_tile, panels, width, col_tiles, tile_count, capacity, slots)
    chunks = panels * col_tiles
    relayed = len(detour_chunks(chunks))
    any_spec = pl.BlockSpec(memory_space=pl.ANY)
    smem_spec = pl.BlockSpec(memory_space=pltpu.SMEM)
    dma = pltpu.SemaphoreType.DMA
    result, _ = pl.pallas_call(
        functools.partial(kernel, dims),
        out_shape=(
            jax.ShapeDtypeStruct((slots, width, width), BF16),
            jax.ShapeDtypeStruct((n_sub, *meta.shape), jnp.int32),
        ),
        in_specs=[smem_spec, any_spec, any_spec, any_spec, any_spec, any_spec],
        out_specs=(pl.BlockSpec(memory_space=pltpu.VMEM), any_spec),
        scratch_shapes=[
            pltpu.VMEM(lower_blocks.shape, BF16),
            pltpu.VMEM(inverse.shape, F32),
            pltpu.VMEM(right_cols.shape, BF16),
            pltpu.VMEM((slots, width, width), BF16),
            pltpu.VMEM((2, col_tiles, width, width), F32),
            pltpu.VMEM((n_tile * panels, col_tiles, width, width), BF16),
            pltpu.VMEM((relayed, width, width), BF16),
            pltpu.VMEM((n_sub, capacity, width, width), BF16),
            pltpu.VMEM((n_sub - 1, capacity, width, width), BF16),
            pltpu.VMEM((slots, width, width), F32),
            pltpu.SMEM((n_sub * capacity,), jnp.int32),
            pltpu.SMEM((n_sub * capacity,), jnp.int32),
            pltpu.SMEM((n_sub, *meta.shape), jnp.int32),
            dma((6,)),
            dma((panels,)),
            dma((panels,)),
            dma((chunks,)),
            dma((chunks,)),
            dma((chunks,)),
            dma((chunks,)),
            dma((relayed,)),
            dma((relayed,)),
            dma((relayed,)),
            dma((relayed,)),
            dma((n_sub, capacity)),
            dma((n_sub, capacity)),
            dma((n_sub,)),
            dma((n_sub,)),
            dma((3,)),
        ],
        compiler_params=pltpu.CompilerParams(
            collective_id=0, has_side_effects=True, vmem_limit_bytes=50 * 1024 * 1024
        ),
    )(meta, meta, lower_blocks, inverse, right_cols, base[0])
    return result[None]


def solution(mesh):
    placed = (
        P("sub", None, None, None),
        P("sub", None, None, None),
        P("sub", None, "tile"),
        P("sub", None, "tile"),
        P("sub", None, "tile"),
        P("sub", "tile", None, None),
    )
    return jax.shard_map(
        shards, mesh=mesh, in_specs=placed, out_specs=P("sub", "tile", None, None), check_vma=False
    )
```
